32 devices in a mesh: dp: 8 (over y, x, core), tensor: 4 (over z).
Axes of the slice: x: 2, y: 2, z: 4, core: 2. Of those that a mesh axis runs over, the one named last changes fastest.
Arguments:
- layer_input: bfloat16 [16384, 4096], P('dp', 'tensor'), may hold values from -54 to 54
- queries: bfloat16 [16384, 2048], P('dp', 'tensor'), may hold values from -6 to 6
- keys_values: bfloat16 [16384, 2, 1024], P('dp', None, 'tensor'), may hold values from -6 to 6
- out_grads: bfloat16 [16384, 2048], P('dp', 'tensor'), may hold values from -6 to 6
- log_sums: bfloat16 [16384, 16], P('dp', 'tensor'), may hold values from 2.5 to 5.5
- deltas: bfloat16 [16384, 16], P('dp', 'tensor'), may hold values from -1.5 to 1.5
- tile_fill: int32 [8, 16], replicated, may hold values from 1 to 128, as said below
- tile_cont: int32 [8, 16], replicated, may hold values from 0 to 1, as said below
- moment_first: float32 [4096, 2, 1024], P(('tensor', 'dp')), may hold values from -2 to 2
- moment_second: float32 [2, 8], replicated, may hold values from 0.05 to 0.5
Outputs:
- update: float32 [4096, 2, 1024], P(('tensor', 'dp'))
- new_first: float32 [4096, 2, 1024], P(('tensor', 'dp'))
- new_second: float32 [2, 8], replicated
The draws below stay inside these ranges and needn't reach their ends.
Inputs may be any that keep to these rules, and one draw needn't show every extreme that they name: `tile_fill`: a tile followed by a tile with tile_cont 1 has all 128 positions live. Documents span one or two tiles: tile_cont is 0 for the first tile of each group and never 1 for two tiles in a row.
All inputs are finite; a program needn't handle non-finite values.
Results may differ from the reference program's by a relative error of at most 0.0055.
Values may be sent and summed in bfloat16 or wider, within the bound.
A program may use at most 64 MiB of HBM per device.

```python
import math
import jax
import jax.numpy as jnp
from jax import lax

D = 4096
HQ = 16
HK = 8
HD = 128
BLK = 128
TILES_DEV = 16
TOKENS = 16384
N_DP = 8


def tile_layout(key):
    key = jax.random.fold_in(key, 7)
    key_bits, key_fill = jax.random.split(key)
    coin_bits = jax.random.randint(key_bits, (N_DP, TILES_DEV), 0, 2)
    tile_index = jnp.arange(TILES_DEV)

    def advance(previous, column):
        col_bits, position = column
        linked = jnp.where(position == 1, 1, jnp.where(position == 0, 0, col_bits * (1 - previous)))
        linked = linked.astype(jnp.int32)
        return (linked, linked)
    final_state, linked = lax.scan(advance, jnp.zeros((N_DP,), jnp.int32), (coin_bits.T, tile_index))
    tile_cont = linked.T.astype(jnp.int32)
    following = jnp.concatenate([tile_cont[:, 1:], jnp.zeros_like(tile_cont[:, :1])], 1)
    raw_fill = jax.random.randint(key_fill, (N_DP, TILES_DEV), 1, BLK + 1)
    tile_fill = jnp.where(following == 1, BLK, raw_fill).astype(jnp.int32)
    return (tile_fill, tile_cont)


def draw_tile_fill(key, part):
    return tile_layout(key)[0]


def draw_tile_cont(key, part):
    return tile_layout(key)[1]


def draw_layer_input(key, part):
    key = jax.random.fold_in(key, 11)
    key_cols, key_vals = jax.random.split(key, 2)
    columns = jnp.arange(D, dtype=jnp.float32) / D
    spread = jnp.exp(jax.random.uniform(key_cols, (D,), jnp.float32, math.log(0.3), math.log(3.0)))
    col_ramp = 1.0 + 2.0 * columns
    base_vals = jnp.clip(jax.random.normal(key_vals, (TOKENS, D), jnp.float32), -6.0, 6.0)
    return (base_vals * spread[None, :] * col_ramp[None, :]).astype(jnp.bfloat16)


def steps_of(rng, extent, shards, smallest, largest):
    gain, own = 1.0, jax.random.fold_in(rng, 6)
    for dim, shards_of in shards:
        draws = jnp.exp(jax.random.uniform(jax.random.fold_in(own, dim), (shards_of,), jnp.float32, smallest / len(shards), largest / len(shards)))
        gain = gain * jnp.repeat(draws, extent[dim] // shards_of).reshape([-1 if axis == dim else 1 for axis in range(len(extent))])
    return gain


def scatter_about(own_key, shape, scale, reach, pieces=(), held_as=jnp.bfloat16):
    drawn = jax.random.normal(own_key, shape, jnp.float32) * scale
    if len(pieces) > 0:
        drawn = steps_of(own_key, shape, pieces, -0.22, 0.18) * drawn
    return jnp.clip(drawn, min=-reach, max=reach).astype(held_as)


def setup_inputs(seed: int = 0) -> dict:
    arg_keys = jax.random.split(jax.random.key(seed), 11)
    layer_input = draw_layer_input(jax.random.fold_in(arg_keys[10], 71), 0)
    queries = scatter_about(arg_keys[1], (TOKENS, HQ * HD), 1.0, 6.0, ((0, 8), (1, 4)))
    keys_values = scatter_about(arg_keys[2], (TOKENS, 2, HK * HD), 1.0, 6.0, ((0, 8), (2, 4)))
    out_grads = scatter_about(arg_keys[3], (TOKENS, HQ * HD), 1.0, 6.0, ((0, 8), (1, 4)))
    log_sums = jnp.clip(2.5 + 3.0 * jax.random.uniform(arg_keys[4], (TOKENS, HQ), jnp.float32) ** steps_of(arg_keys[4], (TOKENS, HQ), ((0, 8), (1, 4)), -0.2, 0.2), 2.5, 5.5).astype(jnp.bfloat16)
    deltas = scatter_about(arg_keys[5], (TOKENS, HQ), 0.3, 1.5, ((0, 8), (1, 4)))
    tile_fill = draw_tile_fill(jax.random.fold_in(arg_keys[10], 71), 0)
    tile_cont = draw_tile_cont(jax.random.fold_in(arg_keys[10], 71), 0)
    moment_first = scatter_about(arg_keys[8], (D, 2, HK * HD), 0.3, 2.0, ((0, 32),), jnp.float32)
    moment_second = jnp.clip(jnp.exp(jax.random.uniform(arg_keys[9], (2, HK), jnp.float32, math.log(0.05), math.log(0.5))), 0.05, 0.5)
    return {"layer_input": layer_input, "queries": queries, "keys_values": keys_values, "out_grads": out_grads, "log_sums": log_sums, "deltas": deltas, "tile_fill": tile_fill, "tile_cont": tile_cont, "moment_first": moment_first, "moment_second": moment_second}


HIGHEST_PRECISION = lax.Precision.HIGHEST

def band_grads(q_tiles, k_tiles, v_tiles, do_tiles, lse_tiles, delta_tiles, fill_tiles, cont_tiles):
    tile_total, block_len, groups, head_width = q_tiles.shape
    scale_qk = head_width ** (-0.5)
    q_full = q_tiles.astype(jnp.float32)
    do_full = do_tiles.astype(jnp.float32)
    k_full = k_tiles.astype(jnp.float32)
    v_full = v_tiles.astype(jnp.float32)
    zero_tile = jnp.zeros_like(k_full[:1])
    k_window = jnp.concatenate([jnp.concatenate([zero_tile, k_full[:-1]], 0), k_full], 1)
    v_window = jnp.concatenate([jnp.concatenate([zero_tile, v_full[:-1]], 0), v_full], 1)
    places = jnp.arange(block_len)
    live_rows = places[None, :] < fill_tiles[:, None]
    causal = places[:, None] >= places[None, :]
    own_part = live_rows[:, :, None] & causal[None]
    prev_part = live_rows[:, :, None] & (cont_tiles[:, None, None] == 1) & (places[None, None, :] >= 0)
    allowed = jnp.concatenate([prev_part, own_part], 2)[:, None]
    scores = jnp.einsum('sqgd,skd->sgqk', q_full, k_window, precision=HIGHEST_PRECISION) * scale_qk
    lse_rows = jnp.swapaxes(lse_tiles.astype(jnp.float32), 1, 2)[..., None]
    delta_rows = jnp.swapaxes(delta_tiles.astype(jnp.float32), 1, 2)[..., None]
    prob_vals = jnp.where(allowed, jnp.exp(scores - lse_rows), 0.0)
    dprobs = jnp.einsum('sqgd,skd->sgqk', do_full, v_window, precision=HIGHEST_PRECISION)
    dscores = prob_vals * (dprobs - delta_rows)
    prob_half = lax.optimization_barrier(prob_vals.astype(jnp.bfloat16)).astype(jnp.float32)
    score_half = lax.optimization_barrier(dscores.astype(jnp.bfloat16)).astype(jnp.float32)
    value_grad = jnp.einsum('sgqk,sqgd->skd', prob_half, do_full, precision=HIGHEST_PRECISION)
    key_grad = jnp.einsum('sgqk,sqgd->skd', score_half, q_full, precision=HIGHEST_PRECISION) * scale_qk
    key_out = key_grad[:, block_len:] + jnp.concatenate([key_grad[1:, :block_len], jnp.zeros_like(key_grad[:1, :block_len])], 0)
    value_out = value_grad[:, block_len:] + jnp.concatenate([value_grad[1:, :block_len], jnp.zeros_like(value_grad[:1, :block_len])], 0)
    return (key_out, value_out)

def reference(layer_input, queries, keys_values, out_grads, log_sums, deltas, tile_fill, tile_cont, moment_first, moment_second):
    tiles_all = N_DP * TILES_DEV
    groups = HQ // HK
    q_heads = queries.reshape(tiles_all, BLK, HK, groups, HD).transpose(2, 0, 1, 3, 4)
    do_heads = out_grads.reshape(tiles_all, BLK, HK, groups, HD).transpose(2, 0, 1, 3, 4)
    k_heads = keys_values[:, 0].reshape(tiles_all, BLK, HK, HD).transpose(2, 0, 1, 3)
    v_heads = keys_values[:, 1].reshape(tiles_all, BLK, HK, HD).transpose(2, 0, 1, 3)
    lse_heads = log_sums.reshape(tiles_all, BLK, HK, groups).transpose(2, 0, 1, 3)
    delta_heads = deltas.reshape(tiles_all, BLK, HK, groups).transpose(2, 0, 1, 3)
    fill_flat = tile_fill.reshape(-1)
    cont_flat = tile_cont.reshape(-1)

    def one_head(operands):
        q_one, k_one, v_one, do_one, lse_one, delta_one = operands
        key_out, value_out = band_grads(q_one, k_one, v_one, do_one, lse_one, delta_one, fill_flat, cont_flat)
        return jnp.stack([key_out, value_out], 2).astype(jnp.bfloat16)
    per_head = lax.map(one_head, (q_heads, k_heads, v_heads, do_heads, lse_heads, delta_heads))
    kv_grads = per_head.transpose(1, 2, 3, 0, 4).reshape(TOKENS, 2 * HK * HD)
    summed = lax.dot_general(layer_input, kv_grads, (((0,), (0,)), ((), ())), preferred_element_type=jnp.float32)
    proj_grads = summed.reshape(D, 2, HK * HD) / math.sqrt(TOKENS)
    new_first = 0.9 * moment_first + (1 - 0.9) * proj_grads
    squares = lax.optimization_barrier(jnp.sum(jnp.square(proj_grads).reshape(D, 2, HK, HD), axis=(0, 3)))
    new_second = 0.95 * moment_second + (1 - 0.95) * squares / (D * HD)
    step_size = jnp.sqrt(new_second / (1 - 0.95 ** 2)) + 1e-08
    update = ((new_first / (1 - 0.9 ** 2)).reshape(D, 2, HK, HD) / step_size[None, :, :, None]).reshape(D, 2, HK * HD)
    return (update, new_first, new_second)
```

```python
import functools
import math

import jax
import jax.numpy as jnp
from jax import lax
from jax.experimental import pallas as pl
from jax.experimental.pallas import tpu as pltpu
from jax.sharding import PartitionSpec as P

D = 4096
HD = 128

ADAM_ONE = 0.9
ADAM_TWO = 0.95
ADAM_EPS = 1e-08
MESH = pl.DeviceIdType.MESH
NT = (((1,), (1,)), ((), ()))


def attend_kernel(tiles, group_size, fill_ref, cont_ref, q_ref, k_ref, v_ref, do_ref, lse_ref, delta_ref, out_ref):
    group = lax.axis_index("dp")
    block = k_ref.shape[0] // tiles
    scale_qk = HD ** (-0.5)
    wide = 2 * group_size * block
    key_place = lax.broadcasted_iota(jnp.int32, (block, wide), 0)
    column = lax.broadcasted_iota(jnp.int32, (block, wide), 1)
    query_place = column % block
    is_next = column >= group_size * block

    def one_tile(tile, carry):
        after = jnp.minimum(tile + 1, tiles - 1)
        here = pl.ds(pl.multiple_of(tile * block, block), block)
        there = pl.ds(pl.multiple_of(after * block, block), block)
        fill_here = fill_ref[group, tile]
        fill_there = jnp.where(tile + 1 < tiles, fill_ref[group, after] * (cont_ref[group, after] == 1).astype(jnp.int32), 0)
        heads = [slice(h * HD, (h + 1) * HD) for h in range(group_size)]
        q_cat = jnp.concatenate([q_ref[w, h] for w in (here, there) for h in heads], 0)
        do_cat = jnp.concatenate([do_ref[w, h] for w in (here, there) for h in heads], 0)
        lse = jnp.concatenate([lse_ref[0, h : h + 1, w] for w in (here, there) for h in range(group_size)], 1)
        delta = jnp.concatenate([delta_ref[0, h : h + 1, w] for w in (here, there) for h in range(group_size)], 1)
        scores = lax.dot_general(k_ref[here, :], q_cat, NT, preferred_element_type=jnp.float32) * scale_qk
        limit = jnp.where(is_next, fill_there, fill_here)
        allowed = (query_place < limit) & (is_next | (query_place >= key_place))
        prob = jnp.where(allowed, jnp.exp(scores - lse), 0.0)
        dprob = lax.dot_general(v_ref[here, :], do_cat, NT, preferred_element_type=jnp.float32)
        dscore = prob * (dprob - delta)
        value_grad = jnp.dot(prob.astype(jnp.bfloat16), do_cat, preferred_element_type=jnp.float32)
        key_grad = jnp.dot(dscore.astype(jnp.bfloat16), q_cat, preferred_element_type=jnp.float32) * scale_qk
        out_ref[0, here, :] = key_grad.astype(jnp.bfloat16)
        out_ref[1, here, :] = value_grad.astype(jnp.bfloat16)
        return carry

    lax.fori_loop(0, tiles, one_tile, 0, unroll=2)


def attend(queries, keys, values, out_grads, lse_rows, delta_rows, tile_fill, tile_cont):
    tokens = queries.shape[0]
    kv_local = keys.shape[1] // HD
    group_size = queries.shape[1] // keys.shape[1]
    tiles = tile_fill.shape[1]
    smem = pl.BlockSpec(memory_space=pltpu.SMEM)
    q_spec = pl.BlockSpec((tokens, group_size * HD), lambda h: (0, h))
    k_spec = pl.BlockSpec((tokens, HD), lambda h: (0, h))
    row_spec = pl.BlockSpec((1, group_size, tokens), lambda h: (h, 0, 0))
    return pl.pallas_call(
        functools.partial(attend_kernel, tiles, group_size),
        grid=(kv_local,),
        out_shape=jax.ShapeDtypeStruct((2 * kv_local, tokens, HD), jnp.bfloat16),
        in_specs=[smem, smem, q_spec, k_spec, k_spec, q_spec, row_spec, row_spec],
        out_specs=pl.BlockSpec((2, tokens, HD), lambda h: (h, 0, 0)),
        compiler_params=pltpu.CompilerParams(vmem_limit_bytes=32 * 2**20),
    )(tile_fill, tile_cont, queries, keys, values, out_grads, lse_rows, delta_rows)


def sum_kernel(
    groups, planes, inv, kv_ref, layer_ref, out_ref, sq_ref,
    layer, flipped, gathered, terms, pair_send, pair_recv, chip_send, chip_recv, sq_groups, sq_mid, sq_planes,
    load_sem, kv_right, kv_left, kv_recv, pair_ssem, pair_rsem, chip_ssem, chip_rsem,
    sqg_ssem, sqg_rsem, sqp_ssem, sqp_rsem,
):
    me, plane = lax.axis_index("dp"), lax.axis_index("tensor")
    chips = groups // 2
    chip, core = me // 2, me % 2
    partner = me + 1 - 2 * core
    chunks, tokens, _ = kv_ref.shape
    rows = layer_ref.shape[1]
    rows_out = rows // groups

    load = pltpu.make_async_copy(layer_ref, layer, load_sem)
    load.start()

    barrier = pltpu.get_barrier_semaphore()
    for step in range(1, groups):
        pl.semaphore_signal(barrier, inc=1, device_id=(lax.rem(me + step, groups), plane), device_id_type=MESH)
    for step in range(1, planes):
        pl.semaphore_signal(barrier, inc=1, device_id=(me, lax.rem(plane + step, planes)), device_id_type=MESH)
    pl.semaphore_wait(barrier, groups + planes - 2)

    def to_right(source, c, p):
        return pltpu.make_async_remote_copy(
            src_ref=source, dst_ref=gathered.at[c, p], send_sem=kv_right.at[c, p], recv_sem=kv_recv.at[c, p],
            device_id=(me, jnp.minimum(plane + 1, planes - 1)), device_id_type=MESH,
        )

    def to_left(source, c, p):
        return pltpu.make_async_remote_copy(
            src_ref=source, dst_ref=gathered.at[c, p], send_sem=kv_left.at[c, p], recv_sem=kv_recv.at[c, p],
            device_id=(me, jnp.maximum(plane - 1, 0)), device_id_type=MESH,
        )

    def send_own(c):
        @pl.when(plane < planes - 1)
        def _():
            to_right(kv_ref.at[c], c, plane).start()

        @pl.when(plane > 0)
        def _():
            to_left(kv_ref.at[c], c, plane).start()

    row_block = min(256, rows)

    def product(piece_ref, c, p):
        def one(i, carry):
            at = pl.ds(pl.multiple_of(i * row_block, row_block), row_block)
            terms[c, p, at, :] = jnp.dot(flipped[at, :], piece_ref[...], preferred_element_type=jnp.float32)
            return carry

        lax.fori_loop(0, rows // row_block, one, 0)

    def slice_of(k, parity):
        return pl.ds(pl.multiple_of((2 * k + parity) * rows_out, rows_out), rows_out)

    def pair_copy(c):
        return pltpu.make_async_remote_copy(
            src_ref=pair_send.at[c], dst_ref=pair_recv.at[c], send_sem=pair_ssem.at[c], recv_sem=pair_rsem.at[c],
            device_id=(partner, plane), device_id_type=MESH,
        )

    def chip_copy(c, step):
        other = lax.rem(chip + step, chips)
        return pltpu.make_async_remote_copy(
            src_ref=chip_send.at[c, step - 1], dst_ref=chip_recv.at[c, step - 1],
            send_sem=chip_ssem.at[c, step - 1], recv_sem=chip_rsem.at[c, step - 1],
            device_id=(2 * other + core, plane), device_id_type=MESH,
        )

    def stage_one(c):
        for k in range(chips):
            pair_send[c, k] = terms[c, :, slice_of(k, 1 - core), :].astype(jnp.bfloat16)
        pair_copy(c).start()

    def stage_two(c):
        pair_copy(c).wait_recv()
        for step in range(1, chips):
            other = lax.rem(chip + step, chips)
            both = terms[c, :, slice_of(other, core), :] + pair_recv[c, other].astype(jnp.float32)
            chip_send[c, step - 1] = both.astype(jnp.bfloat16)
            chip_copy(c, step).start()

    def stage_three(c):
        total = terms[c, :, slice_of(chip, core), :] + pair_recv[c, chip].astype(jnp.float32)
        for step in range(1, chips):
            chip_copy(c, step).wait_recv()
            total = total + chip_recv[c, step - 1].astype(jnp.float32)
        total = total * inv
        out_ref[c] = total
        squares = jnp.sum(total * total, axis=1)
        sq_groups[me, c] = squares

    send_own(0)
    load.wait()
    flip_block = min(128, rows)

    def flip(i, carry):
        at = pl.ds(pl.multiple_of(i * flip_block, flip_block), flip_block)
        flipped[at, :] = layer[:, at].T
        return carry

    lax.fori_loop(0, rows // flip_block, flip, 0)

    def one_chunk(c, carry):
        product(kv_ref.at[c], c, plane)
        for dist in range(1, planes):
            left, right = plane - dist, plane + dist

            @pl.when(left >= 0)
            def _():
                to_right(kv_ref.at[c], c, left).wait_recv()

                @pl.when(plane < planes - 1)
                def _():
                    to_right(gathered.at[c, left], c, left).start()

            @pl.when(right < planes)
            def _():
                to_left(kv_ref.at[c], c, right).wait_recv()

                @pl.when(plane > 0)
                def _():
                    to_left(gathered.at[c, right], c, right).start()

            if dist == 1:
                @pl.when(c + 1 < chunks)
                def _():
                    send_own(c + 1)

            @pl.when(left >= 0)
            def _():
                product(gathered.at[c, left], c, left)

            @pl.when(right < planes)
            def _():
                product(gathered.at[c, right], c, right)

            if dist == 1:
                @pl.when(c > 0)
                def _():
                    stage_two(c - 1)

            if dist == min(2, planes - 1):
                @pl.when(c > 0)
                def _():
                    stage_three(c - 1)

        stage_one(c)
        return carry

    lax.fori_loop(0, chunks, one_chunk, 0)
    stage_two(chunks - 1)
    stage_three(chunks - 1)

    def sq_group_copy(step):
        return pltpu.make_async_remote_copy(
            src_ref=sq_groups.at[me], dst_ref=sq_groups.at[me], send_sem=sqg_ssem.at[step - 1],
            recv_sem=sqg_rsem.at[step - 1],
            device_id=(lax.rem(me + step, groups), plane), device_id_type=MESH,
        )

    for step in range(1, groups):
        sq_group_copy(step).start()
    for step in range(1, groups):
        sq_group_copy(step).wait_recv()
    sq_mid[...] = sq_groups[0]
    for g in range(1, groups):
        sq_mid[...] += sq_groups[g]
    sq_planes[plane] = sq_mid[...]

    def sq_plane_copy(step):
        return pltpu.make_async_remote_copy(
            src_ref=sq_mid, dst_ref=sq_planes.at[plane], send_sem=sqp_ssem.at[step - 1],
            recv_sem=sqp_rsem.at[step - 1],
            device_id=(me, lax.rem(plane + step, planes)), device_id_type=MESH,
        )

    for step in range(1, planes):
        sq_plane_copy(step).start()
    for step in range(1, planes):
        sq_plane_copy(step).wait_recv()
    summed = sq_planes[0]
    for p in range(1, planes):
        summed = summed + sq_planes[p]
    sq_ref[...] = summed

    for step in range(1, groups):
        sq_group_copy(step).wait_send()
    for step in range(1, planes):
        sq_plane_copy(step).wait_send()

    def drain(c, carry):
        pair_copy(c).wait_send()
        for step in range(1, chips):
            chip_copy(c, step).wait_send()
        for p in range(planes):
            @pl.when((plane < planes - 1) & (p <= plane))
            def _():
                to_right(kv_ref.at[c], c, p).wait_send()

            @pl.when((plane > 0) & (p >= plane))
            def _():
                to_left(kv_ref.at[c], c, p).wait_send()
        return carry

    lax.fori_loop(0, chunks, drain, 0)


def sum_over_groups(kv_chunks, layer_input, groups, planes):
    chunks, tokens, _ = kv_chunks.shape
    rows = layer_input.shape[1]
    rows_out = rows // groups
    chips = groups // 2
    half, full = jnp.bfloat16, jnp.float32
    dma = pltpu.SemaphoreType.DMA
    vmem = pl.BlockSpec(memory_space=pltpu.VMEM)
    return pl.pallas_call(
        functools.partial(sum_kernel, groups, planes, 1.0 / math.sqrt(tokens * groups)),
        out_shape=(
            jax.ShapeDtypeStruct((chunks, planes, rows_out, HD), full),
            jax.ShapeDtypeStruct((chunks, planes, HD), full),
        ),
        in_specs=[vmem, pl.BlockSpec(memory_space=pl.ANY)],
        out_specs=(vmem, vmem),
        scratch_shapes=[
            pltpu.VMEM((tokens, rows), half),
            pltpu.VMEM((rows, tokens), half),
            pltpu.VMEM((chunks, planes, tokens, HD), half),
            pltpu.VMEM((chunks, planes, rows, HD), full),
            pltpu.VMEM((chunks, chips, planes, rows_out, HD), half),
            pltpu.VMEM((chunks, chips, planes, rows_out, HD), half),
            pltpu.VMEM((chunks, chips - 1, planes, rows_out, HD), half),
            pltpu.VMEM((chunks, chips - 1, planes, rows_out, HD), half),
            pltpu.VMEM((groups, chunks, planes, HD), full),
            pltpu.VMEM((chunks, planes, HD), full),
            pltpu.VMEM((planes, chunks, planes, HD), full),
            dma,
            dma((chunks, planes)),
            dma((chunks, planes)),
            dma((chunks, planes)),
            dma((chunks,)),
            dma((chunks,)),
            dma((chunks, chips - 1)),
            dma((chunks, chips - 1)),
            dma((groups - 1,)),
            dma((groups - 1,)),
            dma((planes - 1,)),
            dma((planes - 1,)),
        ],
        compiler_params=pltpu.CompilerParams(
            collective_id=0, has_side_effects=True, vmem_limit_bytes=56 * 2**20
        ),
    )(kv_chunks, layer_input)


def per_device(
    layer_input, queries, keys_values, out_grads, log_sums, deltas, tile_fill, tile_cont, moment_first, moment_second
):
    groups, planes = lax.axis_size("dp"), lax.axis_size("tensor")
    keys, values = keys_values[:, 0], keys_values[:, 1]
    tokens = queries.shape[0]
    kv_local = keys.shape[1] // HD
    lse_rows = log_sums.astype(jnp.float32).T.reshape(kv_local, -1, tokens)
    delta_rows = deltas.astype(jnp.float32).T.reshape(kv_local, -1, tokens)
    kv_chunks = attend(queries, keys, values, out_grads, lse_rows, delta_rows, tile_fill, tile_cont)
    summed, lane_squares = sum_over_groups(kv_chunks, layer_input, groups, planes)
    rows_out = summed.shape[2]
    heads_kv = moment_second.shape[1]
    parts = summed.reshape(kv_local, 2, planes, rows_out, HD)
    proj_grads = parts.transpose(3, 1, 2, 0, 4).reshape(rows_out, 2, -1)
    squares = jnp.sum(lane_squares.reshape(kv_local, 2, planes, HD), 3).transpose(1, 2, 0).reshape(2, heads_kv)
    new_first = ADAM_ONE * moment_first + (1 - ADAM_ONE) * proj_grads
    new_second = ADAM_TWO * moment_second + (1 - ADAM_TWO) * squares / (D * HD)
    step_size = jnp.sqrt(new_second / (1 - ADAM_TWO**2)) + ADAM_EPS
    scaled = (new_first / (1 - ADAM_ONE**2)).reshape(rows_out, 2, heads_kv, -1)
    update = (scaled / step_size[None, :, :, None]).reshape(proj_grads.shape)
    return (update, new_first, new_second)


def solution(mesh):
    in_specs = (
        P("dp", "tensor"),
        P("dp", "tensor"),
        P("dp", None, "tensor"),
        P("dp", "tensor"),
        P("dp", "tensor"),
        P("dp", "tensor"),
        P(),
        P(),
        P(("tensor", "dp"), None, None),
        P(),
    )
    out_specs = (P(("tensor", "dp"), None, None), P(("tensor", "dp"), None, None), P())
    return jax.shard_map(
        per_device, mesh=mesh, in_specs=in_specs, out_specs=out_specs, check_vma=False
    )
```
